512 devices in a mesh: sector: 32 (over y, x, core), term: 16 (over z).
Axes of the slice: x: 4, y: 4, z: 16, core: 2. Of those that a mesh axis runs over, the one named last changes fastest.
Arguments:
- blocks: bfloat16 [20480, 640], P('sector'), may hold values from -6 to 6
- left_env: bfloat16 [32, 16, 640, 1920], P('sector', 'term'), may hold values from -0.125 to 0.125
- right_env: bfloat16 [32, 16, 640, 640], P('sector', 'term'), may hold values from -0.0625 to 0.0625
- coupling: int32 [32, 3], P('sector'), may hold values 0 or 1
- widths: int32 [32], P('sector'), may hold values from 320 to 640
Outputs:
- filtered: bfloat16 [20480, 640], P('sector')
The draws below stay inside these ranges and needn't reach their ends.
All inputs are finite; a program needn't handle non-finite values. No bound on the sum of `coupling` on one device may be relied on, other than what follows from the above.
Results may differ from the reference program's by a relative error of at most 0.005.
Values may be sent and summed in bfloat16 or wider, within the bound.
No kernel may reach another device: no remote copies, remote signals or barrier semaphores. Data moves between devices by JAX's collectives and lax.ppermute only.
A program may use at most 64 MiB of HBM per device.

```python
import jax
import jax.numpy as jnp
from jax import lax

P_SIZE = 640
COUPLED = 3
SECTORS = 32
TERMS = 16


def with_ends(entries, key, least, high):
    shape = entries.shape
    index_at = [jax.random.randint(jax.random.fold_in(key, axis), (), 0, shape[axis]) for axis in range(len(shape))]
    entries = entries.at[tuple(index_at)].set(least)
    longest = shape.index(max(shape))
    index_at[longest] = (index_at[longest] + 1) % shape[longest]
    return entries.at[tuple(index_at)].set(high)


def block_scale(own_key, dims, cuts, low, largest):
    def one(dim, shards_of):
        draws = jax.random.uniform(jax.random.fold_in(jax.random.fold_in(own_key, 6), dim), (shards_of,), jnp.float32, low / len(cuts), largest / len(cuts))
        return jnp.repeat(jnp.exp(draws), dims[dim] // shards_of).reshape((-1,) + (1,) * (len(dims) - dim - 1))

    factor_of = one(*cuts[0])
    for cut in cuts[1:]:
        factor_of = factor_of * one(*cut)
    return factor_of


def scatter_about(rng, extent, scale, most, cuts=(), kind=jnp.bfloat16):
    loudness = block_scale(rng, extent, cuts, -0.22, 0.18) if cuts else 1.0
    drawn = jax.random.normal(rng, extent, jnp.float32) * scale * loudness
    return jnp.minimum(jnp.maximum(drawn, -most), most).astype(kind)


def setup_inputs(seed: int = 0) -> dict:
    key_list = jax.random.split(jax.random.key(seed), 6)
    blocks = scatter_about(key_list[0], (SECTORS * P_SIZE, P_SIZE), 1.0, 6.0, ((0, 32),))
    left_env = scatter_about(key_list[1], (SECTORS, TERMS, P_SIZE, COUPLED * P_SIZE), (COUPLED * P_SIZE) ** -0.5, 0.125, ((0, 32), (1, 16)))
    right_env = scatter_about(key_list[2], (SECTORS, TERMS, P_SIZE, P_SIZE), (P_SIZE * TERMS) ** -0.5, 0.0625, ((0, 32), (1, 16)))
    coupling = with_ends((jax.random.randint(key_list[3], (SECTORS, COUPLED), 0, 4) < 3).astype(jnp.int32), jax.random.fold_in(key_list[3], 1), 0, 1)
    widths = with_ends(jax.random.randint(key_list[4], (SECTORS,), P_SIZE // 2, P_SIZE + 1), jax.random.fold_in(key_list[4], 1), P_SIZE // 2, P_SIZE).astype(jnp.int32)
    return dict(blocks=blocks, left_env=left_env, right_env=right_env, coupling=coupling, widths=widths)


def keep_live(values, live_width, row_offset):
    row_index = row_offset + lax.broadcasted_iota(jnp.int32, values.shape, 0)
    col_index = lax.broadcasted_iota(jnp.int32, values.shape, 1)
    return jnp.where((row_index < live_width) & (col_index < live_width), values, jnp.zeros_like(values))


def apply_operator(source, left_env, right_env, coupling, widths):
    zero_block = jnp.zeros((1, P_SIZE, P_SIZE), source.dtype)
    padded = jnp.concatenate([zero_block, source, zero_block], axis=0)
    nearby = jnp.stack([padded[:-2], padded[1:-1], padded[2:]], axis=1)

    def per_sector(pieces):
        left_part, right_part, nearby_part, coupled, live_width = pieces
        scaled = nearby_part * coupled.astype(source.dtype)[:, None, None]
        stacked = scaled.reshape(COUPLED * P_SIZE, P_SIZE).astype(jnp.float32)
        partial_value = jnp.einsum("tik,kj->tij", left_part.astype(jnp.float32), stacked).astype(jnp.bfloat16)
        summed = jnp.einsum("tij,tjl->il", partial_value.astype(jnp.float32), right_part.astype(jnp.float32))
        return keep_live(summed, live_width, 0)

    return lax.map(per_sector, (left_env, right_env, nearby, coupling, widths))


def reference(blocks, left_env, right_env, coupling, widths):
    source = blocks.reshape(SECTORS, P_SIZE, P_SIZE)
    first_pass = apply_operator(source, left_env, right_env, coupling, widths).astype(jnp.bfloat16)
    second = apply_operator(first_pass, left_env, right_env, coupling, widths)
    filtered = (2.0 * second - source.astype(jnp.float32)).astype(jnp.bfloat16)
    return filtered.reshape(SECTORS * P_SIZE, P_SIZE)
```

```python
import jax
import jax.numpy as jnp
from jax import lax
from jax.sharding import PartitionSpec as P


def with_halo(x, axis):
    count = lax.axis_size(axis)
    up = [(i, (i + 1) % count) for i in range(count - 1)]
    down = [(j, i) for i, j in up]
    before = lax.ppermute(x, axis, up)
    after = lax.ppermute(x, axis, down)
    return jnp.concatenate([before, x, after], axis=0)


def keep_live(values, live_width, row_offset):
    row_index = row_offset + lax.broadcasted_iota(jnp.int32, values.shape, 0)
    col_index = lax.broadcasted_iota(jnp.int32, values.shape, 1)
    return jnp.where(
        (row_index < live_width) & (col_index < live_width), values, jnp.zeros_like(values)
    )


def contract(stacked, left_part, right_part):
    partial_value = jnp.einsum(
        "ik,kj->ij", left_part, stacked, preferred_element_type=jnp.float32
    ).astype(jnp.bfloat16)
    return jnp.einsum("ij,jl->il", partial_value, right_part, preferred_element_type=jnp.float32)


def shards(blocks, left_env, right_env, coupling, widths):
    side = blocks.shape[1]
    left_part = left_env[0, 0]
    right_part = right_env[0, 0]
    live_width = widths[0]
    row_scale = jnp.repeat(coupling[0].astype(jnp.bfloat16), side)
    terms = lax.axis_size("term")
    rows = side // terms
    row_offset = lax.axis_index("term") * rows

    def apply_rows(source):
        nearby = with_halo(source, "sector")
        part = contract(nearby * row_scale[:, None], left_part, right_part)
        part = part.astype(jnp.bfloat16).reshape(terms, rows, side)
        pieces = lax.all_to_all(part, "term", 0, 0, tiled=True)
        total = jnp.sum(pieces.astype(jnp.float32), axis=0)
        return keep_live(total, live_width, row_offset)

    def gather(piece):
        return lax.all_gather(piece, "term", axis=0, tiled=True)

    first_pass = gather(apply_rows(blocks).astype(jnp.bfloat16))
    own = lax.dynamic_slice_in_dim(blocks, row_offset, rows, axis=0).astype(jnp.float32)
    return gather((2.0 * apply_rows(first_pass) - own).astype(jnp.bfloat16))


def solution(mesh):
    placed = (
        P("sector", None),
        P("sector", "term", None, None),
        P("sector", "term", None, None),
        P("sector", None),
        P("sector"),
    )
    return jax.shard_map(
        shards, mesh=mesh, in_specs=placed, out_specs=P("sector", None), check_vma=False
    )
```

```python
import jax
import jax.numpy as jnp
from jax import lax
from jax.sharding import PartitionSpec as P


def with_halo(x, axis):
    count = lax.axis_size(axis)
    up = [(i, (i + 1) % count) for i in range(count - 1)]
    down = [(j, i) for i, j in up]
    before = lax.ppermute(x, axis, up)
    after = lax.ppermute(x, axis, down)
    return jnp.concatenate([before, x, after], axis=0)


def keep_live(values, live_width, row_offset):
    row_index = row_offset + lax.broadcasted_iota(jnp.int32, values.shape, 0)
    col_index = lax.broadcasted_iota(jnp.int32, values.shape, 1)
    return jnp.where(
        (row_index < live_width) & (col_index < live_width), values, jnp.zeros_like(values)
    )


def contract(stacked, left_part, right_part):
    partial_value = jnp.einsum(
        "ik,kj->ij", left_part, stacked, preferred_element_type=jnp.float32
    ).astype(jnp.bfloat16)
    return jnp.einsum("ij,jl->il", partial_value, right_part, preferred_element_type=jnp.float32)


def shards(blocks, left_env, right_env, coupling, widths):
    side = blocks.shape[1]
    left_part = left_env[0, 0]
    right_part = right_env[0, 0]
    live_width = widths[0]
    row_scale = jnp.repeat(coupling[0].astype(jnp.bfloat16), side)

    def live_part(source):
        nearby = with_halo(source, "sector")
        return keep_live(contract(nearby * row_scale[:, None], left_part, right_part), live_width, 0)

    first_pass = lax.psum(live_part(blocks), "term").astype(jnp.bfloat16)
    once = jnp.where(lax.axis_index("term") == 0, 1.0, 0.0)
    second = 2.0 * live_part(first_pass) - once * blocks.astype(jnp.float32)
    return lax.psum(second, "term").astype(jnp.bfloat16)


def solution(mesh):
    placed = (
        P("sector", None),
        P("sector", "term", None, None),
        P("sector", "term", None, None),
        P("sector", None),
        P("sector"),
    )
    return jax.shard_map(
        shards, mesh=mesh, in_specs=placed, out_specs=P("sector", None), check_vma=False
    )
```

```python
import functools

import jax
import jax.numpy as jnp
from jax import lax
from jax.experimental import pallas as pl
from jax.experimental.pallas import tpu as pltpu
from jax.sharding import PartitionSpec as P


ROW_STEPS = 2


def early_body(where, coupled, left_own, own, left_mate, mate, total):
    mate_at = where[0]
    own_part = jnp.dot(left_own[...], own[...], preferred_element_type=jnp.float32)
    mate_part = jnp.dot(left_mate[...], mate[...], preferred_element_type=jnp.float32)
    total[...] = (
        coupled[1].astype(jnp.float32) * own_part
        + coupled[mate_at].astype(jnp.float32) * mate_part
    )


def late_body(where, coupled, width, early, left_far, far, right, *rest, second):
    far_at = 2 - where[0]
    live_width = width[0]
    out = rest[-1]
    far_part = jnp.dot(left_far[...], far[...], preferred_element_type=jnp.float32)
    partial = (early[...] + coupled[far_at].astype(jnp.float32) * far_part).astype(jnp.bfloat16)
    summed = jnp.dot(partial, right[...], preferred_element_type=jnp.float32)
    rows = summed.shape[0]
    row_index = pl.program_id(0) * rows + lax.broadcasted_iota(jnp.int32, summed.shape, 0)
    col_index = lax.broadcasted_iota(jnp.int32, summed.shape, 1)
    live = (row_index < live_width) & (col_index < live_width)
    summed = jnp.where(live, summed, jnp.zeros_like(summed))
    if second:
        once = where[1].astype(jnp.float32)
        summed = 2.0 * summed - once * rest[0][...].astype(jnp.float32)
    out[...] = summed


def early_product(where, coupled, left_part, own, mate):
    side = own.shape[1]
    whole = lambda i, where, coupled: (0, 0)
    return pl.pallas_call(
        early_body,
        grid_spec=pltpu.PrefetchScalarGridSpec(
            num_scalar_prefetch=2,
            grid=(1,),
            in_specs=[
                pl.BlockSpec((side, side), lambda i, where, coupled: (0, 1)),
                pl.BlockSpec((side, side), whole),
                pl.BlockSpec((side, side), lambda i, where, coupled: (0, where[0])),
                pl.BlockSpec((side, side), whole),
            ],
            out_specs=pl.BlockSpec((side, side), whole),
        ),
        out_shape=jax.ShapeDtypeStruct((side, side), jnp.float32),
        cost_estimate=pl.CostEstimate(
            flops=4 * side**3, bytes_accessed=12 * side * side, transcendentals=0
        ),
        name="early_product",
    )(where, coupled, left_part, own, left_part, mate)


def late_product(where, coupled, width, early, left_part, far, right_part, base=None):
    side = far.shape[1]
    rows = side // ROW_STEPS
    whole = lambda i, *_: (0, 0)
    by_rows = pl.BlockSpec((rows, side), lambda i, *_: (i, 0))
    in_specs = [
        by_rows,
        pl.BlockSpec((rows, side), lambda i, where, *_: (i, 2 - where[0])),
        pl.BlockSpec((side, side), whole),
        pl.BlockSpec((side, side), whole),
    ]
    operands = [early, left_part, far, right_part]
    if base is not None:
        in_specs.append(by_rows)
        operands.append(base)
    return pl.pallas_call(
        functools.partial(late_body, second=base is not None),
        grid_spec=pltpu.PrefetchScalarGridSpec(
            num_scalar_prefetch=3, grid=(ROW_STEPS,), in_specs=in_specs, out_specs=by_rows
        ),
        out_shape=jax.ShapeDtypeStruct((side, side), jnp.float32),
        cost_estimate=pl.CostEstimate(
            flops=4 * side**3, bytes_accessed=16 * side * side, transcendentals=0
        ),
        name="late_product",
    )(where, coupled, width, *operands)


def shards(blocks, left_env, right_env, coupling, widths):
    left_part = left_env[0, 0]
    right_part = right_env[0, 0]
    coupled = coupling[0]
    count = lax.axis_size("sector")
    sector = lax.axis_index("sector")
    mate_at = jnp.where(sector % 2 == 0, 2, 0).astype(jnp.int32)
    once = (lax.axis_index("term") == 0).astype(jnp.int32)
    where = jnp.stack([mate_at, once])
    across = [(i, i + 1) for i in range(1, count - 1, 2)]
    across += [(j, i) for i, j in across]
    within = [(i, i ^ 1) for i in range(count)]

    def live_part(source, base=None):
        far = lax.ppermute(source, "sector", across)
        mate = lax.ppermute(source, "sector", within)
        early = early_product(where, coupled, left_part, source, mate)
        return late_product(where, coupled, widths, early, left_part, far, right_part, base)

    first_pass = lax.psum(live_part(blocks), "term").astype(jnp.bfloat16)
    return lax.psum(live_part(first_pass, blocks), "term").astype(jnp.bfloat16)


def solution(mesh):
    placed = (
        P("sector", None),
        P("sector", "term", None, None),
        P("sector", "term", None, None),
        P("sector", None),
        P("sector"),
    )
    return jax.shard_map(
        shards, mesh=mesh, in_specs=placed, out_specs=P("sector", None), check_vma=False
    )
```

```python
import jax
import jax.numpy as jnp
from jax import lax
from jax.sharding import PartitionSpec as P


def keep_live(values, live_width):
    row_index = lax.broadcasted_iota(jnp.int32, values.shape, 0)
    col_index = lax.broadcasted_iota(jnp.int32, values.shape, 1)
    return jnp.where(
        (row_index < live_width) & (col_index < live_width), values, jnp.zeros_like(values)
    )


def dot(a, b):
    return jnp.dot(a, b, preferred_element_type=jnp.float32)


def shards(blocks, left_env, right_env, coupling, widths):
    side = blocks.shape[1]
    left_part = left_env[0, 0]
    right_part = right_env[0, 0]
    coupled = coupling[0].astype(jnp.bfloat16)
    live_width = widths[0]
    count = lax.axis_size("sector")
    mate_at = jnp.where(lax.axis_index("sector") % 2 == 0, 2, 0).astype(jnp.int32)
    once = jnp.where(lax.axis_index("term") == 0, 1.0, 0.0)
    across = [(i, i + 1) for i in range(1, count - 1, 2)]
    across += [(j, i) for i, j in across]
    within = [(i, i ^ 1) for i in range(count)]

    def left_of(at):
        piece = lax.dynamic_slice(left_part, (0, at * side), (side, side))
        return piece * lax.dynamic_index_in_dim(coupled, at, keepdims=False)

    left_near = jnp.concatenate([left_of(1), left_of(mate_at)], axis=1)
    left_far = left_of(2 - mate_at)
    left_near, left_far = lax.optimization_barrier((left_near, left_far))

    def live_part(source):
        far = lax.ppermute(source, "sector", across)
        mate = lax.ppermute(source, "sector", within)
        early = dot(left_near, jnp.concatenate([source, mate], axis=0))
        early = lax.optimization_barrier(early)
        partial = (early + dot(left_far, far)).astype(jnp.bfloat16)
        return keep_live(dot(partial, right_part), live_width)

    first_pass = lax.psum(live_part(blocks), "term").astype(jnp.bfloat16)
    second = 2.0 * live_part(first_pass) - once * blocks.astype(jnp.float32)
    return lax.psum(second, "term").astype(jnp.bfloat16)


def solution(mesh):
    placed = (
        P("sector", None),
        P("sector", "term", None, None),
        P("sector", "term", None, None),
        P("sector", None),
        P("sector"),
    )
    return jax.shard_map(
        shards, mesh=mesh, in_specs=placed, out_specs=P("sector", None), check_vma=False
    )
```

```python
import jax
import jax.numpy as jnp
from jax import lax
from jax.experimental import pallas as pl
from jax.experimental.pallas import tpu as pltpu
from jax.sharding import PartitionSpec as P


def keep_live(values, live_width):
    row_index = lax.broadcasted_iota(jnp.int32, values.shape, 0)
    col_index = lax.broadcasted_iota(jnp.int32, values.shape, 1)
    return jnp.where(
        (row_index < live_width) & (col_index < live_width), values, jnp.zeros_like(values)
    )


def dot(a, b):
    return jnp.dot(a, b, preferred_element_type=jnp.float32)


def mate_place():
    return 2 - 2 * (lax.axis_index("sector") % 2)


CUT_STEPS = 5


def cut_body(coupled, left, near, far):
    side = far.shape[1]
    mate_first = mate_place() == 0

    def piece(at):
        scale = coupled[at].astype(jnp.float32)
        columns = left[:, at * side : (at + 1) * side].astype(jnp.float32)
        return (columns * scale).astype(left.dtype)

    before, after = piece(0), piece(2)
    near[:, :side] = piece(1)
    near[:, side:] = jnp.where(mate_first, before, after)
    far[...] = jnp.where(mate_first, after, before)


def cut(left_part, coupled):
    side, width = left_part.shape
    rows = side // CUT_STEPS

    def by_rows(columns):
        return pl.BlockSpec((rows, columns), lambda i, coupled: (i, 0))

    return pl.pallas_call(
        cut_body,
        grid_spec=pltpu.PrefetchScalarGridSpec(
            num_scalar_prefetch=1,
            grid=(CUT_STEPS,),
            in_specs=[by_rows(width)],
            out_specs=(by_rows(2 * side), by_rows(side)),
        ),
        out_shape=(
            jax.ShapeDtypeStruct((side, 2 * side), left_part.dtype),
            jax.ShapeDtypeStruct((side, side), left_part.dtype),
        ),
        name="cut",
    )(coupled, left_part)


def shards(blocks, left_env, right_env, coupling, widths):
    right_part = right_env[0, 0]
    live_width = widths[0]
    count = lax.axis_size("sector")
    once = jnp.where(lax.axis_index("term") == 0, 1.0, 0.0)
    across = [(i, i + 1) for i in range(1, count - 1, 2)]
    across += [(j, i) for i, j in across]
    within = [(i, i ^ 1) for i in range(count)]
    left_near, left_far = cut(left_env[0, 0], coupling[0])

    def live_part(source):
        far = lax.ppermute(source, "sector", across)
        mate = lax.ppermute(source, "sector", within)
        near = jnp.concatenate([source, mate], axis=0)
        early = lax.optimization_barrier(dot(left_near, near))
        partial = (early + dot(left_far, far)).astype(jnp.bfloat16)
        return keep_live(dot(partial, right_part), live_width)

    first_pass = lax.psum(live_part(blocks), "term").astype(jnp.bfloat16)
    second = 2.0 * live_part(first_pass) - once * blocks.astype(jnp.float32)
    return lax.psum(second, "term").astype(jnp.bfloat16)


def solution(mesh):
    placed = (
        P("sector", None),
        P("sector", "term", None, None),
        P("sector", "term", None, None),
        P("sector", None),
        P("sector"),
    )
    return jax.shard_map(
        shards, mesh=mesh, in_specs=placed, out_specs=P("sector", None), check_vma=False
    )
```

```python
import jax
import jax.numpy as jnp
from jax import lax
from jax.experimental import pallas as pl
from jax.experimental.pallas import tpu as pltpu
from jax.sharding import PartitionSpec as P


def keep_live(values, live_width):
    row_index = lax.broadcasted_iota(jnp.int32, values.shape, 0)
    col_index = lax.broadcasted_iota(jnp.int32, values.shape, 1)
    return jnp.where(
        (row_index < live_width) & (col_index < live_width), values, jnp.zeros_like(values)
    )


def dot(a, b):
    return jnp.dot(a, b, preferred_element_type=jnp.float32)


def mate_place():
    return 2 - 2 * (lax.axis_index("sector") % 2)


CUT_STEPS = 5
FIRST_ROWS = 384


def cut_body(coupled, left, near, far):
    side = far.shape[1]
    mate_at = mate_place()

    def piece(at):
        scale = jnp.full((1, side), coupled[at].astype(jnp.float32)).astype(left.dtype)
        return left[:, pl.ds(pl.multiple_of(at * side, 128), side)] * scale

    near[:, :side] = piece(1)
    near[:, side:] = piece(mate_at)
    far[...] = piece(2 - mate_at)


def cut(left_part, coupled):
    side, width = left_part.shape
    rows = side // CUT_STEPS

    def by_rows(columns):
        return pl.BlockSpec((rows, columns), lambda i, coupled: (i, 0))

    return pl.pallas_call(
        cut_body,
        grid_spec=pltpu.PrefetchScalarGridSpec(
            num_scalar_prefetch=1,
            grid=(CUT_STEPS,),
            in_specs=[by_rows(width)],
            out_specs=(by_rows(2 * side), by_rows(side)),
        ),
        out_shape=(
            jax.ShapeDtypeStruct((side, 2 * side), left_part.dtype),
            jax.ShapeDtypeStruct((side, side), left_part.dtype),
        ),
        name="cut",
    )(coupled, left_part)


def shards(blocks, left_env, right_env, coupling, widths):
    right_part = right_env[0, 0]
    live_width = widths[0]
    count = lax.axis_size("sector")
    once = jnp.where(lax.axis_index("term") == 0, 1.0, 0.0)
    across = [(i, i + 1) for i in range(1, count - 1, 2)]
    across += [(j, i) for i, j in across]
    within = [(i, i ^ 1) for i in range(count)]
    left_near, left_far = cut(left_env[0, 0], coupling[0])

    def live_part(source, split):
        far = [None, None]
        far[0] = lax.ppermute(source[:split], "sector", across)
        if split < source.shape[0]:
            far[1] = lax.ppermute(source[split:], "sector", across)
        mate = lax.ppermute(source, "sector", within)
        near = jnp.concatenate([source, mate], axis=0)
        early = lax.optimization_barrier(dot(left_near, near))
        left_last = left_far
        if far[1] is not None:
            early, first = lax.optimization_barrier((early, far[0]))
            early += lax.optimization_barrier(dot(left_far[:, :split], first))
            left_last = left_far[:, split:]
        last = far[0] if far[1] is None else far[1]
        partial = (early + dot(left_last, last)).astype(jnp.bfloat16)
        return keep_live(dot(partial, right_part), live_width)

    first_pass = lax.psum(live_part(blocks, blocks.shape[0]), "term").astype(jnp.bfloat16)
    second = 2.0 * live_part(first_pass, FIRST_ROWS) - once * blocks.astype(jnp.float32)
    return lax.psum(second, "term").astype(jnp.bfloat16)


def solution(mesh):
    placed = (
        P("sector", None),
        P("sector", "term", None, None),
        P("sector", "term", None, None),
        P("sector", None),
        P("sector"),
    )
    return jax.shard_map(
        shards, mesh=mesh, in_specs=placed, out_specs=P("sector", None), check_vma=False
    )
```

```python
import jax
import jax.numpy as jnp
from jax import lax
from jax.experimental import pallas as pl
from jax.experimental.pallas import tpu as pltpu
from jax.sharding import PartitionSpec as P


def keep_live(values, live_width):
    row_index = lax.broadcasted_iota(jnp.int32, values.shape, 0)
    col_index = lax.broadcasted_iota(jnp.int32, values.shape, 1)
    return jnp.where(
        (row_index < live_width) & (col_index < live_width), values, jnp.zeros_like(values)
    )


def dot(a, b):
    return jnp.dot(a, b, preferred_element_type=jnp.float32)


def mate_place():
    return 2 - 2 * (lax.axis_index("sector") % 2)


CUT_STEPS = 5


def cut_body(coupled, left, near, far, held, arrived, left_us):
    side = far.shape[1]
    rows = side // CUT_STEPS
    mate_at = mate_place()
    places = (1, mate_at, 2 - mate_at)
    chunks = [(step, piece) for step in range(CUT_STEPS) for piece in range(len(places))]

    def copy_in(step, piece):
        at = pl.ds(step * rows, rows)
        columns = pl.ds(pl.multiple_of(places[piece] * side, 128), side)
        return pltpu.make_async_copy(
            left.at[at, columns], held.at[piece, at, :], arrived.at[step, piece]
        )

    def copy_out(step, piece):
        at = pl.ds(step * rows, rows)
        target = far.at[at, :] if piece == 2 else near.at[at, pl.ds(piece * side, side)]
        return pltpu.make_async_copy(held.at[piece, at, :], target, left_us.at[step, piece])

    for chunk in chunks:
        copy_in(*chunk).start()
    for step, piece in chunks:
        copy_in(step, piece).wait()
        at = pl.ds(step * rows, rows)
        scale = jnp.full((1, side), coupled[places[piece]].astype(jnp.float32))
        held[piece, at, :] = held[piece, at, :] * scale.astype(held.dtype)
        copy_out(step, piece).start()
    for chunk in chunks:
        copy_out(*chunk).wait()


def cut(left_part, coupled):
    side = left_part.shape[0]
    anywhere = pl.BlockSpec(memory_space=pl.ANY)
    return pl.pallas_call(
        cut_body,
        in_specs=[pl.BlockSpec(memory_space=pltpu.SMEM), anywhere],
        out_specs=(anywhere, anywhere),
        out_shape=(
            jax.ShapeDtypeStruct((side, 2 * side), left_part.dtype),
            jax.ShapeDtypeStruct((side, side), left_part.dtype),
        ),
        scratch_shapes=[
            pltpu.VMEM((3, side, side), left_part.dtype),
            pltpu.SemaphoreType.DMA((CUT_STEPS, 3)),
            pltpu.SemaphoreType.DMA((CUT_STEPS, 3)),
        ],
        name="cut",
    )(coupled, left_part)


def shards(blocks, left_env, right_env, coupling, widths):
    right_part = right_env[0, 0]
    live_width = widths[0]
    count = lax.axis_size("sector")
    once = jnp.where(lax.axis_index("term") == 0, 1.0, 0.0)
    across = [(i, i + 1) for i in range(1, count - 1, 2)]
    across += [(j, i) for i, j in across]
    within = [(i, i ^ 1) for i in range(count)]
    left_near, left_far = cut(left_env[0, 0], coupling[0])

    def live_part(source):
        far = lax.ppermute(source, "sector", across)
        mate = lax.ppermute(source, "sector", within)
        near = jnp.concatenate([source, mate], axis=0)
        early = lax.optimization_barrier(dot(left_near, near))
        partial = (early + dot(left_far, far)).astype(jnp.bfloat16)
        return keep_live(dot(partial, right_part), live_width)

    first_pass = lax.psum(live_part(blocks), "term").astype(jnp.bfloat16)
    second = 2.0 * live_part(first_pass) - once * blocks.astype(jnp.float32)
    return lax.psum(second, "term").astype(jnp.bfloat16)


def solution(mesh):
    placed = (
        P("sector", None),
        P("sector", "term", None, None),
        P("sector", "term", None, None),
        P("sector", None),
        P("sector"),
    )
    return jax.shard_map(
        shards, mesh=mesh, in_specs=placed, out_specs=P("sector", None), check_vma=False
    )
```

```python
import jax
import jax.numpy as jnp
from jax import lax
from jax.experimental import pallas as pl
from jax.experimental.pallas import tpu as pltpu
from jax.sharding import PartitionSpec as P


def keep_live(values, live_width):
    row_index = lax.broadcasted_iota(jnp.int32, values.shape, 0)
    col_index = lax.broadcasted_iota(jnp.int32, values.shape, 1)
    return jnp.where(
        (row_index < live_width) & (col_index < live_width), values, jnp.zeros_like(values)
    )


def dot(a, b):
    return jnp.dot(a, b, preferred_element_type=jnp.float32)


def mate_place():
    return 2 - 2 * (lax.axis_index("sector") % 2)


CUT_STEPS = 5


def cut_body(coupled, left, near, far, held, arrived, left_us):
    side = far.shape[1]
    rows = side // CUT_STEPS
    mate_at = mate_place()
    places = (1, mate_at, 2 - mate_at)
    chunks = [(step, piece) for step in range(CUT_STEPS) for piece in range(len(places))]

    def copy_in(step, piece):
        at = pl.ds(step * rows, rows)
        columns = pl.ds(pl.multiple_of(places[piece] * side, 128), side)
        return pltpu.make_async_copy(
            left.at[at, columns], held.at[piece, at, :], arrived.at[step, piece]
        )

    def copy_out(step, piece):
        at = pl.ds(step * rows, rows)
        target = far.at[at, :] if piece == 2 else near.at[at, pl.ds(piece * side, side)]
        return pltpu.make_async_copy(held.at[piece, at, :], target, left_us.at[step, piece])

    for chunk in chunks:
        copy_in(*chunk).start()
    for step, piece in chunks:
        copy_in(step, piece).wait()
        at = pl.ds(step * rows, rows)
        scale = jnp.full((1, side), coupled[places[piece]].astype(jnp.float32))
        held[piece, at, :] = held[piece, at, :] * scale.astype(held.dtype)
        copy_out(step, piece).start()
    for chunk in chunks:
        copy_out(*chunk).wait()


def cut(left_part, coupled):
    side = left_part.shape[0]
    anywhere = pl.BlockSpec(memory_space=pl.ANY)
    return pl.pallas_call(
        cut_body,
        in_specs=[pl.BlockSpec(memory_space=pltpu.SMEM), anywhere],
        out_specs=(anywhere, anywhere),
        out_shape=(
            jax.ShapeDtypeStruct((side, 2 * side), left_part.dtype),
            jax.ShapeDtypeStruct((side, side), left_part.dtype),
        ),
        scratch_shapes=[
            pltpu.VMEM((3, side, side), left_part.dtype),
            pltpu.SemaphoreType.DMA((CUT_STEPS, 3)),
            pltpu.SemaphoreType.DMA((CUT_STEPS, 3)),
        ],
        name="cut",
    )(coupled, left_part)


def shards(blocks, left_env, right_env, coupling, widths):
    right_part = right_env[0, 0]
    live_width = widths[0]
    count = lax.axis_size("sector")
    once = jnp.where(lax.axis_index("term") == 0, 1.0, 0.0)
    across = [(i, i + 1) for i in range(1, count - 1, 2)]
    across += [(j, i) for i, j in across]
    within = [(i, i ^ 1) for i in range(count)]
    left_near, left_far = cut(left_env[0, 0], coupling[0])

    def live_part(source):
        far = lax.ppermute(source, "sector", across)
        side = source.shape[0]
        early, sent = lax.optimization_barrier((dot(left_near[:, :side], source), source))
        mate = lax.ppermute(sent, "sector", within)
        early = lax.optimization_barrier(early + dot(left_near[:, side:], mate))
        partial = (early + dot(left_far, far)).astype(jnp.bfloat16)
        return keep_live(dot(partial, right_part), live_width)

    first_pass = lax.psum(live_part(blocks), "term").astype(jnp.bfloat16)
    second = 2.0 * live_part(first_pass) - once * blocks.astype(jnp.float32)
    return lax.psum(second, "term").astype(jnp.bfloat16)


def solution(mesh):
    placed = (
        P("sector", None),
        P("sector", "term", None, None),
        P("sector", "term", None, None),
        P("sector", None),
        P("sector"),
    )
    return jax.shard_map(
        shards, mesh=mesh, in_specs=placed, out_specs=P("sector", None), check_vma=False
    )
```

```python
import jax
import jax.numpy as jnp
from jax import lax
from jax.experimental import pallas as pl
from jax.experimental.pallas import tpu as pltpu
from jax.sharding import PartitionSpec as P


def keep_live(values, live_width):
    row_index = lax.broadcasted_iota(jnp.int32, values.shape, 0)
    col_index = lax.broadcasted_iota(jnp.int32, values.shape, 1)
    return jnp.where(
        (row_index < live_width) & (col_index < live_width), values, jnp.zeros_like(values)
    )


def dot(a, b):
    return jnp.dot(a, b, preferred_element_type=jnp.float32)


def mate_place():
    return 2 - 2 * (lax.axis_index("sector") % 2)


CUT_STEPS = 5


def cut_body(coupled, left, near, far, held, arrived, left_us):
    side = far.shape[1]
    rows = side // CUT_STEPS
    mate_at = mate_place()
    places = (1, mate_at, 2 - mate_at)
    chunks = [(step, piece) for step in range(CUT_STEPS) for piece in range(len(places))]

    def copy_in(step, piece):
        at = pl.ds(step * rows, rows)
        columns = pl.ds(pl.multiple_of(places[piece] * side, 128), side)
        return pltpu.make_async_copy(
            left.at[at, columns], held.at[piece, at, :], arrived.at[step, piece]
        )

    def copy_out(step, piece):
        at = pl.ds(step * rows, rows)
        target = far.at[at, :] if piece == 2 else near.at[at, pl.ds(piece * side, side)]
        return pltpu.make_async_copy(held.at[piece, at, :], target, left_us.at[step, piece])

    for chunk in chunks:
        copy_in(*chunk).start()
    for step, piece in chunks:
        copy_in(step, piece).wait()
        at = pl.ds(step * rows, rows)
        scale = jnp.full((1, side), coupled[places[piece]].astype(jnp.float32))
        held[piece, at, :] = held[piece, at, :] * scale.astype(held.dtype)
        copy_out(step, piece).start()
    for chunk in chunks:
        copy_out(*chunk).wait()


def cut(left_part, coupled):
    side = left_part.shape[0]
    anywhere = pl.BlockSpec(memory_space=pl.ANY)
    return pl.pallas_call(
        cut_body,
        in_specs=[pl.BlockSpec(memory_space=pltpu.SMEM), anywhere],
        out_specs=(anywhere, anywhere),
        out_shape=(
            jax.ShapeDtypeStruct((side, 2 * side), left_part.dtype),
            jax.ShapeDtypeStruct((side, side), left_part.dtype),
        ),
        scratch_shapes=[
            pltpu.VMEM((3, side, side), left_part.dtype),
            pltpu.SemaphoreType.DMA((CUT_STEPS, 3)),
            pltpu.SemaphoreType.DMA((CUT_STEPS, 3)),
        ],
        name="cut",
    )(coupled, left_part)


def shards(blocks, left_env, right_env, coupling, widths):
    right_part = right_env[0, 0]
    live_width = widths[0]
    count = lax.axis_size("sector")
    once = jnp.where(lax.axis_index("term") == 0, 1.0, 0.0)
    across = [(i, i + 1) for i in range(1, count - 1, 2)]
    across += [(j, i) for i, j in across]
    within = [(i, i ^ 1) for i in range(count)]
    left_near, left_far = cut(left_env[0, 0], coupling[0])

    def live_part(source):
        far = lax.ppermute(source, "sector", across)
        mate = lax.ppermute(source, "sector", within)
        near = jnp.concatenate([source, mate], axis=0)
        early = lax.optimization_barrier(dot(left_near, near))
        partial = (early + dot(left_far, far)).astype(jnp.bfloat16)
        return keep_live(dot(partial, right_part), live_width)

    part = live_part(blocks)
    half = part.shape[0] // 2
    sums = lax.psum((part[:half], part[half:]), "term")
    first_pass = jnp.concatenate([half_sum.astype(jnp.bfloat16) for half_sum in sums])
    second = 2.0 * live_part(first_pass) - once * blocks.astype(jnp.float32)
    return lax.psum(second, "term").astype(jnp.bfloat16)


def solution(mesh):
    placed = (
        P("sector", None),
        P("sector", "term", None, None),
        P("sector", "term", None, None),
        P("sector", None),
        P("sector"),
    )
    return jax.shard_map(
        shards, mesh=mesh, in_specs=placed, out_specs=P("sector", None), check_vma=False
    )
```
